32 devices in a mesh: groups: 2 (over x), row: 16 (over z, y, core).
Axes of the slice: x: 2, y: 2, z: 4, core: 2. Of those that a mesh axis runs over, the one named last changes fastest.
Arguments:
- design_matrix: bfloat16 [1024, 65536], P('groups', 'row'), parts along dimension 0, may hold values from -0.0546875 to 0.0546875
- targets: float32 [1024, 128], P(('groups', 'row')), parts along dimension 0, may hold values from -24 to 24
- linear: float32 [131072, 128], P(('groups', 'row')), parts along dimension 0, may hold values from -24 to 24
- diagonal: float32 [131072], P(('groups', 'row')), parts along dimension 0, may hold values from 0.1 to 2
- lower_code: int32 [131072, 128], P(('groups', 'row')), parts along dimension 0, may hold values from -192 to -17
- upper_code: int32 [131072, 128], P(('groups', 'row')), parts along dimension 0, may hold values from 16 to 191
Outputs:
- box_iterate: float32 [131072, 128], P(('groups', 'row')), parts along dimension 0
- scaled_dual: float32 [131072, 128], P(('groups', 'row')), parts along dimension 0
The draws below stay inside these ranges and needn't reach their ends.
There are 2 independent parts, one for each index of `groups`. The reference program is written for one: setup_inputs(seed, part) draws one part's arguments, and reference() takes and returns one part's arrays. A program takes and returns all parts, laid end to end along the dimension named above; each array names one. Nothing has to cross between parts.
All inputs are finite; a program needn't handle non-finite values.
Results may differ from the reference program's by a relative error of at most 0.00033.
Values may be sent and summed in bfloat16 or wider, within the bound.
A program may use at most 128 MiB of HBM per device.

```python
import math
import jax
import jax.numpy as jnp
from jax import lax

N = 65536
K = 512
S = 128
ITERS = 4
DEPTH = 5


def place_ends(drawn, own_key, least, largest):
    longest = drawn.shape.index(max(drawn.shape))
    spots = []
    for shift in (0, 1):
        where = [jax.random.randint(jax.random.fold_in(own_key, axis), (), 0, length) for axis, length in enumerate(drawn.shape)]
        where[longest] = (where[longest] + shift) % drawn.shape[longest]
        spots.append(tuple(where))
    return drawn.at[spots[0]].set(least).at[spots[1]].set(largest)


def raised(array, key, source, target, shards_of, factor):
    def block_of(position):
        return (jnp.arange(array.shape[position]) // (array.shape[position] // shards_of)).reshape((-1,) + (1,) * (array.ndim - 1 - position))

    near = jax.random.permutation(key, shards_of)[block_of(target)]
    far = (block_of(target) + shards_of // 2) % shards_of
    return jnp.where((block_of(source) == near) | (block_of(source) == far), factor * array, array)


def level_of(key, extent, pieces, smallest, largest):
    loudness = 1.0
    for dim, shards_of in pieces:
        draws = jax.random.uniform(jax.random.fold_in(jax.random.fold_in(key, 6), dim), (shards_of,), jnp.float32, smallest / len(pieces), largest / len(pieces))
        loudness = loudness * jnp.repeat(jnp.exp(draws), extent[dim] // shards_of).reshape((-1,) + (1,) * (len(extent) - 1 - dim))
    return loudness


def gaussian(rng, extent, deviation, bound, shards=(), kind=jnp.bfloat16):
    values = jax.random.normal(rng, extent, jnp.float32) * deviation
    if len(shards) > 0:
        values = level_of(rng, extent, shards, -0.22, 0.18) * values
    return jnp.clip(values, min=-bound, max=bound).astype(kind)


def noise_with(own_key, extent, spread, reach, shards, heavy, held_as=jnp.bfloat16):
    values = spread * jax.random.normal(own_key, extent, jnp.float32)
    if shards:
        values = values * level_of(own_key, extent, shards, -0.22, 0.18)
    return jnp.clip(raised(values, jax.random.fold_in(own_key, 3), *heavy), -reach, reach).astype(held_as)


def setup_inputs(seed: int = 0, part: int = 0) -> dict:
    key_of = jax.random.split(jax.random.key(seed), 7)
    part_keys = jax.random.split(jax.random.fold_in(key_of[6], part), 7)
    design_matrix = noise_with(part_keys[0], (K, N), (max(N // 3, 2 * K)) ** -0.5, 0.0546875, ((1, 16),), (1, 0, 16, 2.0))
    targets = gaussian(part_keys[1], (K, S), 4.0, 24.0, ((0, 16),), jnp.float32)
    linear = gaussian(part_keys[2], (N, S), 4.0, 24.0, ((0, 16),), jnp.float32)
    diagonal = jnp.clip(jnp.exp(math.log(2.0) - 2.9957323 * jax.random.uniform(part_keys[3], (N,), jnp.float32) ** level_of(part_keys[3], (N,), ((0, 16),), -0.2, 0.2)), 0.1, 2.0)
    lower_code = place_ends(jax.random.randint(part_keys[4], (N, S), -192, -16), jax.random.fold_in(part_keys[4], 1), -192, (-16) - 1).astype(jnp.int32)
    upper_code = place_ends(jax.random.randint(part_keys[5], (N, S), 16, 192), jax.random.fold_in(part_keys[5], 1), 16, 191).astype(jnp.int32)
    return {"design_matrix": design_matrix, "targets": targets, "linear": linear, "diagonal": diagonal, "lower_code": lower_code, "upper_code": upper_code}


rho_plus_lip = 7.0


def solve_small(matrix, rhs):
    count = len(rhs)
    table = [list(line) for line in matrix]
    right = list(rhs)
    for p in range(count):
        for i in range(p + 1, count):
            factor = table[i][p] / table[p][p]
            for j in range(p, count):
                table[i][j] = table[i][j] - factor * table[p][j]
            right[i] = right[i] - factor * right[p]
    result = [None] * count
    for i in reversed(range(count)):
        total = right[i]
        for j in range(i + 1, count):
            total = total - table[i][j] * result[j]
        result[i] = total / table[i][i]
    return result


def mix_weights(gram):
    count = len(gram)
    trace = gram[0][0]
    for i in range(1, count):
        trace = trace + gram[i][i]
    shift = 0.01 * trace / count + 1e-6
    matrix = [[gram[i][j] + (shift if i == j else 0.0) for j in range(count)] for i in range(count)]
    solved = solve_small(matrix, [jnp.ones_like(trace)] * count)
    total = solved[0]
    for i in range(1, count):
        total = total + solved[i]
    return [item / total for item in solved]


def reference(design_matrix, targets, linear, diagonal, lower_code, upper_code):
    lower = lower_code.astype(jnp.float32) / 64.0
    upper = upper_code.astype(jnp.float32) / 64.0
    step_size = (1.0 / (rho_plus_lip + diagonal))[:, None]

    def apply_map(state):
        point = state[0] - state[1]
        point_b = point.astype(jnp.bfloat16)
        product = jnp.dot(design_matrix, point_b, preferred_element_type=jnp.float32)
        misfit = (product - targets).astype(jnp.bfloat16)
        gradient = lax.dot_general(design_matrix, misfit, (((0,), (0,)), ((), ())), preferred_element_type=jnp.float32)
        gradient = gradient + diagonal[:, None] * point + linear
        moved = point - step_size * gradient
        boxed = jnp.clip(moved + state[1], lower, upper)
        scaled = state[1] + moved - boxed
        return jnp.stack([boxed, scaled])

    state = jnp.zeros((2,) + linear.shape, jnp.float32)
    hist_mapped = []
    hist_change = []
    for iteration in range(ITERS):
        mapped = apply_map(state)
        hist_mapped.append(mapped)
        hist_change.append(mapped - state)
        if len(hist_mapped) > DEPTH:
            hist_mapped.pop(0)
            hist_change.pop(0)
        stacked = jnp.stack(hist_change)
        whole = jnp.einsum('icns,jcns->ijs', stacked, stacked, precision=lax.Precision.HIGHEST)
        count = len(hist_change)
        gram = [[whole[i, j] for j in range(count)] for i in range(count)]
        alpha = mix_weights(gram)
        combined = alpha[0][None, None, :] * hist_mapped[0]
        for i in range(1, count):
            combined = combined + alpha[i][None, None, :] * hist_mapped[i]
        state = jnp.stack([jnp.clip(combined[0], lower, upper), combined[1]])
    return state[0], state[1]
```

```python
import functools

import jax
import jax.numpy as jnp
from jax import lax
from jax.experimental import pallas as pl
from jax.experimental.pallas import tpu as pltpu
from jax.sharding import PartitionSpec as P

ITERS = 4
TERM = jnp.bfloat16

rho_plus_lip = 7.0


def solve_small(matrix, rhs):
    count = len(rhs)
    table = [list(line) for line in matrix]
    right = list(rhs)
    for p in range(count):
        for i in range(p + 1, count):
            factor = table[i][p] / table[p][p]
            for j in range(p, count):
                table[i][j] = table[i][j] - factor * table[p][j]
            right[i] = right[i] - factor * right[p]
    result = [None] * count
    for i in reversed(range(count)):
        total = right[i]
        for j in range(i + 1, count):
            total = total - table[i][j] * result[j]
        result[i] = total / table[i][i]
    return result


def mix_weights(gram):
    count = len(gram)
    trace = gram[0][0]
    for i in range(1, count):
        trace = trace + gram[i][i]
    shift = 0.01 * trace / count + 1e-06
    matrix = [[gram[i][j] + (shift if i == j else 0.0) for j in range(count)] for i in range(count)]
    solved = solve_small(matrix, [jnp.ones_like(trace)] * count)
    total = solved[0]
    for i in range(1, count):
        total = total + solved[i]
    return [item / total for item in solved]


def peers_of(n, me):
    if n & (n - 1):
        return [(d, lax.rem(me + d, n), lax.rem(me + n - d, n)) for d in range(n - 1, 0, -1)]
    found = []
    for d in range(n - 1, 0, -1):
        peer = me
        bit = 1
        while bit < n:
            if d & bit:
                peer = peer + bit * (1 - 2 * ((me // bit) % 2))
            bit *= 2
        found.append((d, peer, peer))
    return found


def greet(n, peers):
    barrier = pltpu.get_barrier_semaphore()
    for _, peer, _ in peers:
        pl.semaphore_signal(
            barrier,
            inc=1,
            device_id={"row": peer},
            device_id_type=pl.DeviceIdType.MESH,
        )
    return lambda: pl.semaphore_wait(barrier, n - 1)


def send(src, dst, send_sem, recv_sem, peer):
    copy = pltpu.make_async_remote_copy(
        src_ref=src,
        dst_ref=dst,
        send_sem=send_sem,
        recv_sem=recv_sem,
        device_id={"row": peer},
        device_id_type=pl.DeviceIdType.MESH,
    )
    copy.start()
    return copy


def start_spread(peers, me, mine, whole, send_sem, recv_sem):
    copies = [
        send(mine, whole.at[me], send_sem.at[d], recv_sem.at[d], peer) for d, peer, _ in peers
    ]
    whole[me] = mine[...]
    return copies


def finish(copies):
    for copy in copies:
        copy.wait_recv()
    for copy in copies:
        copy.wait_send()


def chunks(local, size, body):
    def step(i, carry):
        body(pl.ds(pl.multiple_of(i * size, size), size))
        return carry

    lax.fori_loop(0, local // size, step, 0)


def column_sum(x):
    return jnp.sum(x.reshape(-1, 8, x.shape[-1]), axis=0)


def clip(x, lower, upper):
    return jnp.minimum(jnp.maximum(x, lower), upper)


def main_kernel(
    n,
    size,
    a_hbm,
    targets_hbm,
    lin_hbm,
    diag_hbm,
    lo_hbm,
    hi_hbm,
    mapped,
    alpha_ref,
    lower,
    upper,
    a_ref,
    at_ref,
    targets_ref,
    lin_ref,
    diag_ref,
    lo_ref,
    hi_ref,
    step_ref,
    z_ref,
    u_ref,
    changes,
    acc,
    sums,
    terms,
    slots,
    mine,
    misfits,
    part,
    parts,
    grams,
    load_sem,
    send_a,
    recv_a,
    send_b,
    recv_b,
    send_c,
    recv_c,
):
    me = lax.axis_index("row")
    peers = peers_of(n, me)
    local = lin_ref.shape[0]
    k = a_ref.shape[0]

    loads = [
        pltpu.make_async_copy(source, target, load_sem.at[i])
        for i, (source, target) in enumerate(
            [
                (targets_hbm, targets_ref),
                (diag_hbm, diag_ref),
                (a_hbm, a_ref),
                (lo_hbm, lo_ref),
                (hi_hbm, hi_ref),
                (lin_hbm, lin_ref),
            ]
        )
    ]
    for load in loads:
        load.start()
    met = greet(n, peers)
    loads[0].wait()
    mine[...] = (0.0 - targets_ref[...]).astype(jnp.bfloat16)
    met()
    copies = start_spread(peers, me, mine, misfits, send_b, recv_b)

    loads[1].wait()
    lanes = diag_ref.shape[1]
    for i in range(diag_ref.shape[0]):
        line = 1.0 / (rho_plus_lip + diag_ref[i : i + 1, :])
        step_ref[i * lanes : (i + 1) * lanes, :] = jnp.broadcast_to(line, (lanes, lanes)).T
    loads[2].wait()

    def flip(at):
        at_ref[at, :] = a_ref[:, at].T

    chunks(local, size, flip)
    loads[3].wait()
    loads[4].wait()

    def bounds(at):
        lower[at, :] = lo_ref[at, :].astype(jnp.float32) * (1.0 / 64.0)
        upper[at, :] = hi_ref[at, :].astype(jnp.float32) * (1.0 / 64.0)

    chunks(local, size, bounds)
    loads[5].wait()
    acc[...] = jnp.zeros_like(acc)
    sums[...] = jnp.zeros_like(sums)
    finish(copies)

    def gradient_of(at):
        return jnp.dot(
            at_ref[at, :], misfits[...].reshape(k, -1), preferred_element_type=jnp.float32
        )

    def add_product(at, point):
        acc[...] += jnp.dot(
            a_ref[:, at], point.astype(jnp.bfloat16), preferred_element_type=jnp.float32
        )

    def start(at):
        moved = 0.0 - step_ref[at, :] * (gradient_of(at) + lin_ref[at, :])
        boxed = clip(moved, lower[at, :], upper[at, :])
        scaled = moved - boxed
        mapped[0, 0, at, :] = boxed
        mapped[0, 1, at, :] = scaled
        sums[ITERS] += column_sum(boxed * boxed + scaled * scaled)
        add_product(at, boxed - scaled)

    chunks(local, size, start)

    for iteration in range(1, ITERS):
        count = iteration + 1
        last = iteration == ITERS - 1
        terms[...] = acc[...].reshape(terms.shape).astype(terms.dtype)
        copies = [
            send(terms.at[peer], slots.at[d - 1], send_a.at[d], recv_a.at[d], peer)
            for d, peer, _ in peers
        ]
        total = terms[me].astype(jnp.float32) - targets_ref[...]
        for copy, (d, _, _) in reversed(list(zip(copies, peers))):
            copy.wait_recv()
            total = total + slots[d - 1].astype(jnp.float32)
        mine[...] = total.astype(jnp.bfloat16)
        spread = start_spread(peers, me, mine, misfits, send_b, recv_b)
        for copy in copies:
            copy.wait_send()
        finish(spread)

        def advance(at):
            if iteration == 1:
                z, u = mapped[0, 0, at, :], mapped[0, 1, at, :]
            else:
                z, u = z_ref[at, :], u_ref[at, :]
            moved = step_ref[at, :] * (
                rho_plus_lip * (z - u) - lin_ref[at, :] - gradient_of(at)
            )
            raw = moved + u
            boxed = clip(raw, lower[at, :], upper[at, :])
            scaled = raw - boxed
            mapped[iteration, 0, at, :] = boxed
            mapped[iteration, 1, at, :] = scaled
            cz, cu = boxed - z, scaled - u
            if not last:
                changes[iteration - 1, 0, at, :] = cz
                changes[iteration - 1, 1, at, :] = cu
            sums[0] += column_sum(cz * mapped[0, 0, at, :] + cu * mapped[0, 1, at, :])
            for i in range(1, iteration):
                sums[i] += column_sum(
                    cz * changes[i - 1, 0, at, :] + cu * changes[i - 1, 1, at, :]
                )
            sums[iteration] += column_sum(cz * cz + cu * cu)

        chunks(local, size, advance)

        kept = list(range(count)) + ([ITERS] if iteration == 1 else [])
        for i in kept:
            row = i if i < ITERS else ITERS - 1
            part[row : row + 1, :] = jnp.sum(sums[i], axis=0, keepdims=True)
        spread = start_spread(peers, me, part, parts, send_c, recv_c)
        sums[...] = jnp.zeros_like(sums)
        acc[...] = jnp.zeros_like(acc)
        finish(spread)
        whole = parts[0]
        for i in range(1, n):
            whole = whole + parts[i]
        grams[iteration - 1] = whole

        gram = [[None] * count for _ in range(count)]
        gram[0][0] = grams[0, ITERS - 1 : ITERS, :]
        for i in range(1, count):
            for j in range(i + 1):
                gram[i][j] = gram[j][i] = grams[i - 1, j : j + 1, :]
        for i, row in enumerate(mix_weights(gram)):
            alpha_ref[i : i + 1, :] = row

        if last:
            break

        def mix(at):
            z = alpha_ref[0:1, :] * mapped[0, 0, at, :]
            u = alpha_ref[0:1, :] * mapped[0, 1, at, :]
            for i in range(1, count):
                z = z + alpha_ref[i : i + 1, :] * mapped[i, 0, at, :]
                u = u + alpha_ref[i : i + 1, :] * mapped[i, 1, at, :]
            z = clip(z, lower[at, :], upper[at, :])
            z_ref[at, :] = z
            u_ref[at, :] = u
            add_product(at, z - u)

        chunks(local, size, mix)


def mix_kernel(size, mapped, alpha_ref, lower, upper, z_hbm, u_hbm, z_ref, u_ref, sem):
    local = lower.shape[0]
    steps = local // size
    copies = []
    for step in range(steps):
        at = pl.ds(step * size, size)
        z = alpha_ref[0:1, :] * mapped[0, 0, at, :]
        u = alpha_ref[0:1, :] * mapped[0, 1, at, :]
        for i in range(1, ITERS):
            z = z + alpha_ref[i : i + 1, :] * mapped[i, 0, at, :]
            u = u + alpha_ref[i : i + 1, :] * mapped[i, 1, at, :]
        z_ref[at, :] = clip(z, lower[at, :], upper[at, :])
        u_ref[at, :] = u
        for j, (src, dst) in enumerate([(z_ref, z_hbm), (u_ref, u_hbm)]):
            copy = pltpu.make_async_copy(src.at[at, :], dst.at[at, :], sem.at[j, step])
            copy.start()
            copies.append(copy)
    for copy in copies:
        copy.wait()


def per_device(n, design_matrix, targets, linear, diagonal, lower_code, upper_code):
    k = design_matrix.shape[0]
    local, s = linear.shape
    kr = k // n
    size = min(512, local)
    big = (local, s)
    lines = diagonal.reshape(local // s, s)
    vmem = pl.BlockSpec(memory_space=pltpu.VMEM)
    hbm = pl.BlockSpec(memory_space=pl.ANY)
    dma = pltpu.SemaphoreType.DMA((n,))
    mapped, alpha, lower, upper = pl.pallas_call(
        functools.partial(main_kernel, n, size),
        in_specs=[hbm] * 6,
        out_specs=[vmem] * 4,
        out_shape=[
            pltpu.VMEM((ITERS, 2, local, s), jnp.float32),
            pltpu.VMEM((8, s), jnp.float32),
            pltpu.VMEM(big, jnp.float32),
            pltpu.VMEM(big, jnp.float32),
        ],
        scratch_shapes=[
            pltpu.VMEM((k, local), jnp.bfloat16),
            pltpu.VMEM((local, k), jnp.bfloat16),
            pltpu.VMEM((kr, s), jnp.float32),
            pltpu.VMEM(big, jnp.float32),
            pltpu.VMEM((local // s, s), jnp.float32),
            pltpu.VMEM(big, jnp.int32),
            pltpu.VMEM(big, jnp.int32),
            pltpu.VMEM(big, jnp.float32),
            pltpu.VMEM(big, jnp.float32),
            pltpu.VMEM(big, jnp.float32),
            pltpu.VMEM((ITERS - 2, 2, local, s), jnp.float32),
            pltpu.VMEM((k, s), jnp.float32),
            pltpu.VMEM((ITERS + 1, 8, s), jnp.float32),
            pltpu.VMEM((n, kr, s), TERM),
            pltpu.VMEM((n - 1, kr, s), TERM),
            pltpu.VMEM((kr, s), jnp.bfloat16),
            pltpu.VMEM((n, kr, s), jnp.bfloat16),
            pltpu.VMEM((ITERS, s), jnp.float32),
            pltpu.VMEM((n, ITERS, s), jnp.float32),
            pltpu.VMEM((ITERS - 1, ITERS, s), jnp.float32),
            pltpu.SemaphoreType.DMA((6,)),
        ]
        + [dma] * 6,
        compiler_params=pltpu.CompilerParams(
            collective_id=0, has_side_effects=True, vmem_limit_bytes=36 * 1024 * 1024
        ),
        name="main",
    )(design_matrix, targets, linear, lines, lower_code, upper_code)
    return pl.pallas_call(
        functools.partial(mix_kernel, size),
        in_specs=[vmem] * 4,
        out_specs=[hbm] * 2,
        out_shape=[jax.ShapeDtypeStruct(big, jnp.float32)] * 2,
        scratch_shapes=[
            pltpu.VMEM(big, jnp.float32),
            pltpu.VMEM(big, jnp.float32),
            pltpu.SemaphoreType.DMA((2, local // size)),
        ],
        compiler_params=pltpu.CompilerParams(vmem_limit_bytes=8 * 1024 * 1024),
        name="last_mix",
    )(mapped, alpha, lower, upper)


def solution(mesh):
    in_specs = (
        P("groups", "row"),
        P(("groups", "row"), None),
        P(("groups", "row"), None),
        P(("groups", "row")),
        P(("groups", "row"), None),
        P(("groups", "row"), None),
    )
    out_specs = (P(("groups", "row"), None), P(("groups", "row"), None))
    return jax.shard_map(
        functools.partial(per_device, mesh.shape["row"]),
        mesh=mesh,
        in_specs=in_specs,
        out_specs=out_specs,
        check_vma=False,
    )
```

```python
import functools

import jax
import jax.numpy as jnp
from jax import lax
from jax.experimental import pallas as pl
from jax.experimental.pallas import tpu as pltpu
from jax.sharding import PartitionSpec as P

ITERS = 4
TERM = jnp.bfloat16

rho_plus_lip = 7.0


def solve_small(matrix, rhs):
    count = len(rhs)
    table = [list(line) for line in matrix]
    right = list(rhs)
    inverse = []
    for p in range(count):
        inverse.append(1.0 / table[p][p])
        for i in range(p + 1, count):
            factor = table[i][p] * inverse[p]
            for j in range(p + 1, count):
                table[i][j] = table[i][j] - factor * table[p][j]
            right[i] = right[i] - factor * right[p]
    result = [None] * count
    for i in reversed(range(count)):
        total = right[i]
        for j in range(i + 1, count):
            total = total - table[i][j] * result[j]
        result[i] = total * inverse[i]
    return result


def mix_weights(gram):
    count = len(gram)
    trace = gram[0][0]
    for i in range(1, count):
        trace = trace + gram[i][i]
    shift = 0.01 * trace / count + 1e-06
    matrix = [[gram[i][j] + (shift if i == j else 0.0) for j in range(count)] for i in range(count)]
    solved = solve_small(matrix, [jnp.ones_like(trace)] * count)
    total = solved[0]
    for i in range(1, count):
        total = total + solved[i]
    scale = 1.0 / total
    return [item * scale for item in solved]


def peers_of(n, me):
    found = []
    for d in range(n - 1, 0, -1):
        peer = me
        bit = 1
        while bit < n:
            if d & bit:
                peer = peer + bit * (1 - 2 * ((me // bit) % 2))
            bit *= 2
        found.append((d, peer))
    return found


def greet(n, peers):
    barrier = pltpu.get_barrier_semaphore()
    for _, peer in peers:
        pl.semaphore_signal(
            barrier,
            inc=1,
            device_id={"row": peer},
            device_id_type=pl.DeviceIdType.MESH,
        )
    return lambda: pl.semaphore_wait(barrier, n - 1)


def send(src, dst, send_sem, recv_sem, peer):
    copy = pltpu.make_async_remote_copy(
        src_ref=src,
        dst_ref=dst,
        send_sem=send_sem,
        recv_sem=recv_sem,
        device_id={"row": peer},
        device_id_type=pl.DeviceIdType.MESH,
    )
    copy.start()
    return copy


def start_spread(peers, me, mine, whole, send_sem, recv_sem):
    copies = [
        send(mine, whole.at[me], send_sem.at[d], recv_sem.at[d], peer) for d, peer in peers
    ]
    whole[me] = mine[...]
    return copies


def finish(copies):
    for copy in copies:
        copy.wait_recv()
    for copy in copies:
        copy.wait_send()


def chunks(local, size, body):
    def step(i, carry):
        body(pl.ds(pl.multiple_of(i * size, size), size))
        return carry

    lax.fori_loop(0, local // size, step, 0)


def column_sum(x):
    return jnp.sum(x.reshape(-1, 8, x.shape[-1]), axis=0)


def clip(x, lower, upper):
    return jnp.minimum(jnp.maximum(x, lower), upper)


def main_kernel(
    n,
    size,
    a_hbm,
    targets_hbm,
    lin_hbm,
    diag_hbm,
    lo_hbm,
    hi_hbm,
    mapped,
    alpha_ref,
    lower,
    upper,
    a_ref,
    at_ref,
    targets_ref,
    lin_ref,
    diag_ref,
    base_ref,
    lo_ref,
    hi_ref,
    step_ref,
    z_ref,
    u_ref,
    changes,
    acc,
    sums,
    terms,
    slots,
    sent,
    running,
    mine,
    misfits,
    part,
    parts,
    grams,
    load_sem,
    send_a,
    recv_a,
    send_b,
    recv_b,
    send_c,
    recv_c,
):
    me = lax.axis_index("row")
    peers = peers_of(n, me)
    local = lin_ref.shape[0]
    k = a_ref.shape[0]

    loads = [
        pltpu.make_async_copy(source, target, load_sem.at[i])
        for i, (source, target) in enumerate(
            [
                (targets_hbm, targets_ref),
                (diag_hbm, diag_ref),
                (a_hbm, a_ref),
                (lo_hbm, lo_ref),
                (hi_hbm, hi_ref),
                (lin_hbm, lin_ref),
            ]
        )
    ]
    for load in loads:
        load.start()
    met = greet(n, peers)
    loads[0].wait()
    mine[...] = (0.0 - targets_ref[...]).astype(jnp.bfloat16)
    met()
    copies = start_spread(peers, me, mine, misfits, send_b, recv_b)

    loads[1].wait()
    lanes = diag_ref.shape[1]
    for i in range(diag_ref.shape[0]):
        line = 1.0 / (rho_plus_lip + diag_ref[i : i + 1, :])
        step_ref[i * lanes : (i + 1) * lanes, :] = jnp.broadcast_to(line, (lanes, lanes)).T
    loads[2].wait()

    def flip(at):
        at_ref[at, :] = a_ref[:, at].T

    chunks(local, size, flip)
    loads[3].wait()
    loads[4].wait()

    def bounds(at):
        lower[at, :] = lo_ref[at, :].astype(jnp.float32) * (1.0 / 64.0)
        upper[at, :] = hi_ref[at, :].astype(jnp.float32) * (1.0 / 64.0)

    chunks(local, size, bounds)
    loads[5].wait()
    acc[...] = jnp.zeros_like(acc)
    sums[...] = jnp.zeros_like(sums)
    half = me // (n // 2)

    def gradient_of(at, which):
        rows = pl.ds(pl.multiple_of(which * (n // 2), n // 2), n // 2)
        columns = pl.ds(pl.multiple_of(which * (k // 2), k // 2), k // 2)
        return jnp.dot(
            at_ref[at, columns],
            misfits[rows].reshape(k // 2, -1),
            preferred_element_type=jnp.float32,
        )

    def add_product(at, point):
        acc[...] += jnp.dot(
            point.astype(jnp.bfloat16).T, at_ref[at, :], preferred_element_type=jnp.float32
        )

    def near(at):
        base_ref[at, :] -= step_ref[at, :] * gradient_of(at, half)

    def gather_near(copies):
        for copy, (d, _) in zip(copies, peers):
            if d < n // 2:
                copy.wait_recv()
        chunks(local, size, near)
        for copy, (d, _) in zip(copies, peers):
            if d >= n // 2:
                copy.wait_recv()

    def raw_of(at):
        return base_ref[at, :] - step_ref[at, :] * gradient_of(at, 1 - half)

    def base(at):
        base_ref[at, :] = 0.0 - step_ref[at, :] * lin_ref[at, :]

    chunks(local, size, base)
    gather_near(copies)

    def start(at):
        raw = raw_of(at)
        boxed = clip(raw, lower[at, :], upper[at, :])
        scaled = raw - boxed
        mapped[0, 0, at, :] = boxed
        mapped[0, 1, at, :] = scaled
        sums[ITERS] += column_sum(boxed * boxed + scaled * scaled)
        add_product(at, boxed - scaled)

    chunks(local, size, start)
    for copy in copies:
        copy.wait_send()

    for iteration in range(1, ITERS):
        count = iteration + 1
        last = iteration == ITERS - 1
        rounded = acc[...].astype(terms.dtype)
        terms[...] = rounded.T.reshape(terms.shape)
        copies = [
            send(terms.at[peer], slots.at[d - 1], send_a.at[d], recv_a.at[d], peer)
            for d, peer in peers
        ]
        if iteration == 1:
            sent[...] = rounded.astype(jnp.float32)
            total = terms[me].astype(jnp.float32) - targets_ref[...]
        else:
            sent[...] += rounded.astype(jnp.float32)
            total = terms[me].astype(jnp.float32) + running[...]
        acc[...] = 0.0 - sent[...]

        def state(at):
            if iteration == 1:
                return mapped[0, 0, at, :], mapped[0, 1, at, :]
            return z_ref[at, :], u_ref[at, :]

        def base(at):
            z, u = state(at)
            base_ref[at, :] = step_ref[at, :] * (rho_plus_lip * (z - u) - lin_ref[at, :]) + u

        chunks(local, size, base)
        for copy, (d, _) in reversed(list(zip(copies, peers))):
            copy.wait_recv()
            total = total + slots[d - 1].astype(jnp.float32)
        running[...] = total
        mine[...] = total.astype(jnp.bfloat16)
        spread = start_spread(peers, me, mine, misfits, send_b, recv_b)
        for copy in copies:
            copy.wait_send()
        gather_near(spread)

        def advance(at):
            z, u = state(at)
            raw = raw_of(at)
            boxed = clip(raw, lower[at, :], upper[at, :])
            scaled = raw - boxed
            mapped[iteration, 0, at, :] = boxed
            mapped[iteration, 1, at, :] = scaled
            cz, cu = boxed - z, scaled - u
            if not last:
                changes[iteration - 1, 0, at, :] = cz
                changes[iteration - 1, 1, at, :] = cu
            sums[0] += column_sum(cz * mapped[0, 0, at, :] + cu * mapped[0, 1, at, :])
            for i in range(1, iteration):
                sums[i] += column_sum(
                    cz * changes[i - 1, 0, at, :] + cu * changes[i - 1, 1, at, :]
                )
            sums[iteration] += column_sum(cz * cz + cu * cu)

        chunks(local, size, advance)
        for copy in spread:
            copy.wait_send()

        kept = list(range(count)) + ([ITERS] if iteration == 1 else [])
        for i in kept:
            row = i if i < ITERS else ITERS - 1
            part[row : row + 1, :] = jnp.sum(sums[i], axis=0, keepdims=True)
        spread = start_spread(peers, me, part, parts, send_c, recv_c)
        sums[...] = jnp.zeros_like(sums)
        finish(spread)
        whole = parts[0]
        for i in range(1, n):
            whole = whole + parts[i]
        grams[iteration - 1] = whole

        gram = [[None] * count for _ in range(count)]
        gram[0][0] = grams[0, ITERS - 1 : ITERS, :]
        for i in range(1, count):
            for j in range(i + 1):
                gram[i][j] = gram[j][i] = grams[i - 1, j : j + 1, :]
        for i, row in enumerate(mix_weights(gram)):
            alpha_ref[i : i + 1, :] = row

        if last:
            break

        def mix(at):
            z = alpha_ref[0:1, :] * mapped[0, 0, at, :]
            u = alpha_ref[0:1, :] * mapped[0, 1, at, :]
            for i in range(1, count):
                z = z + alpha_ref[i : i + 1, :] * mapped[i, 0, at, :]
                u = u + alpha_ref[i : i + 1, :] * mapped[i, 1, at, :]
            z = clip(z, lower[at, :], upper[at, :])
            z_ref[at, :] = z
            u_ref[at, :] = u
            add_product(at, z - u)

        chunks(local, size, mix)


def mix_kernel(size, mapped, alpha_ref, lower, upper, z_hbm, u_hbm, z_ref, u_ref, sem):
    local = lower.shape[0]
    steps = local // size
    copies = []
    for step in range(steps):
        at = pl.ds(step * size, size)
        z = alpha_ref[0:1, :] * mapped[0, 0, at, :]
        u = alpha_ref[0:1, :] * mapped[0, 1, at, :]
        for i in range(1, ITERS):
            z = z + alpha_ref[i : i + 1, :] * mapped[i, 0, at, :]
            u = u + alpha_ref[i : i + 1, :] * mapped[i, 1, at, :]
        z_ref[at, :] = clip(z, lower[at, :], upper[at, :])
        u_ref[at, :] = u
        for j, (src, dst) in enumerate([(z_ref, z_hbm), (u_ref, u_hbm)]):
            copy = pltpu.make_async_copy(src.at[at, :], dst.at[at, :], sem.at[j, step])
            copy.start()
            copies.append(copy)
    for copy in copies:
        copy.wait()


def per_device(n, design_matrix, targets, linear, diagonal, lower_code, upper_code):
    k = design_matrix.shape[0]
    local, s = linear.shape
    kr = k // n
    size = min(2048, local)
    big = (local, s)
    lines = diagonal.reshape(local // s, s)
    vmem = pl.BlockSpec(memory_space=pltpu.VMEM)
    hbm = pl.BlockSpec(memory_space=pl.ANY)
    dma = pltpu.SemaphoreType.DMA((n,))
    mapped, alpha, lower, upper = pl.pallas_call(
        functools.partial(main_kernel, n, size),
        in_specs=[hbm] * 6,
        out_specs=[vmem] * 4,
        out_shape=[
            pltpu.VMEM((ITERS, 2, local, s), jnp.float32),
            pltpu.VMEM((8, s), jnp.float32),
            pltpu.VMEM(big, jnp.float32),
            pltpu.VMEM(big, jnp.float32),
        ],
        scratch_shapes=[
            pltpu.VMEM((k, local), jnp.bfloat16),
            pltpu.VMEM((local, k), jnp.bfloat16),
            pltpu.VMEM((kr, s), jnp.float32),
            pltpu.VMEM(big, jnp.float32),
            pltpu.VMEM((local // s, s), jnp.float32),
            pltpu.VMEM(big, jnp.float32),
            pltpu.VMEM(big, jnp.int32),
            pltpu.VMEM(big, jnp.int32),
            pltpu.VMEM(big, jnp.float32),
            pltpu.VMEM(big, jnp.float32),
            pltpu.VMEM(big, jnp.float32),
            pltpu.VMEM((ITERS - 2, 2, local, s), jnp.float32),
            pltpu.VMEM((s, k), jnp.float32),
            pltpu.VMEM((ITERS + 1, 8, s), jnp.float32),
            pltpu.VMEM((n, kr, s), TERM),
            pltpu.VMEM((n - 1, kr, s), TERM),
            pltpu.VMEM((s, k), jnp.float32),
            pltpu.VMEM((kr, s), jnp.float32),
            pltpu.VMEM((kr, s), jnp.bfloat16),
            pltpu.VMEM((n, kr, s), jnp.bfloat16),
            pltpu.VMEM((ITERS, s), jnp.float32),
            pltpu.VMEM((n, ITERS, s), jnp.float32),
            pltpu.VMEM((ITERS - 1, ITERS, s), jnp.float32),
            pltpu.SemaphoreType.DMA((6,)),
        ]
        + [dma] * 6,
        compiler_params=pltpu.CompilerParams(
            collective_id=0, has_side_effects=True, vmem_limit_bytes=38 * 1024 * 1024
        ),
        name="main",
    )(design_matrix, targets, linear, lines, lower_code, upper_code)
    return pl.pallas_call(
        functools.partial(mix_kernel, size),
        in_specs=[vmem] * 4,
        out_specs=[hbm] * 2,
        out_shape=[jax.ShapeDtypeStruct(big, jnp.float32)] * 2,
        scratch_shapes=[
            pltpu.VMEM(big, jnp.float32),
            pltpu.VMEM(big, jnp.float32),
            pltpu.SemaphoreType.DMA((2, local // size)),
        ],
        compiler_params=pltpu.CompilerParams(vmem_limit_bytes=8 * 1024 * 1024),
        name="last_mix",
    )(mapped, alpha, lower, upper)


def solution(mesh):
    in_specs = (
        P("groups", "row"),
        P(("groups", "row"), None),
        P(("groups", "row"), None),
        P(("groups", "row")),
        P(("groups", "row"), None),
        P(("groups", "row"), None),
    )
    out_specs = (P(("groups", "row"), None), P(("groups", "row"), None))
    return jax.shard_map(
        functools.partial(per_device, mesh.shape["row"]),
        mesh=mesh,
        in_specs=in_specs,
        out_specs=out_specs,
        check_vma=False,
    )
```

```python
import functools

import jax
import jax.numpy as jnp
from jax import lax
from jax.experimental import pallas as pl
from jax.experimental.pallas import tpu as pltpu
from jax.sharding import PartitionSpec as P

ITERS = 4
TERM = jnp.bfloat16

rho_plus_lip = 7.0


def solve_small(matrix, rhs):
    count = len(rhs)
    table = [list(line) for line in matrix]
    right = list(rhs)
    inverse = []
    for p in range(count):
        inverse.append(1.0 / table[p][p])
        for i in range(p + 1, count):
            factor = table[i][p] * inverse[p]
            for j in range(p + 1, count):
                table[i][j] = table[i][j] - factor * table[p][j]
            right[i] = right[i] - factor * right[p]
    result = [None] * count
    for i in reversed(range(count)):
        total = right[i]
        for j in range(i + 1, count):
            total = total - table[i][j] * result[j]
        result[i] = total * inverse[i]
    return result


def mix_weights(gram):
    count = len(gram)
    trace = gram[0][0]
    for i in range(1, count):
        trace = trace + gram[i][i]
    shift = 0.01 * trace / count + 1e-06
    matrix = [[gram[i][j] + (shift if i == j else 0.0) for j in range(count)] for i in range(count)]
    solved = solve_small(matrix, [jnp.ones_like(trace)] * count)
    total = solved[0]
    for i in range(1, count):
        total = total + solved[i]
    scale = 1.0 / total
    return [item * scale for item in solved]


def peers_of(n, me):
    found = []
    for d in range(n - 1, 0, -1):
        peer = me
        bit = 1
        while bit < n:
            if d & bit:
                peer = peer + bit * (1 - 2 * ((me // bit) % 2))
            bit *= 2
        found.append((d, peer))
    return found


def greet(n, peers):
    barrier = pltpu.get_barrier_semaphore()
    for _, peer in peers:
        pl.semaphore_signal(
            barrier,
            inc=1,
            device_id={"row": peer},
            device_id_type=pl.DeviceIdType.MESH,
        )
    return lambda: pl.semaphore_wait(barrier, n - 1)


def send(src, dst, send_sem, recv_sem, peer):
    copy = pltpu.make_async_remote_copy(
        src_ref=src,
        dst_ref=dst,
        send_sem=send_sem,
        recv_sem=recv_sem,
        device_id={"row": peer},
        device_id_type=pl.DeviceIdType.MESH,
    )
    copy.start()
    return copy


def start_spread(peers, me, mine, whole, send_sem, recv_sem):
    copies = [
        send(mine, whole.at[me], send_sem.at[d], recv_sem.at[d], peer) for d, peer in peers
    ]
    whole[me] = mine[...]
    return copies


def finish(copies):
    for copy in copies:
        copy.wait_recv()
    for copy in copies:
        copy.wait_send()


def chunks(local, size, body):
    def step(i, carry):
        body(pl.ds(pl.multiple_of(i * size, size), size))
        return carry

    lax.fori_loop(0, local // size, step, 0)


def pieces(local, size, body):
    for i in range(local // size):
        body(pl.ds(i * size, size))


def column_sum(x):
    return jnp.sum(x.reshape(-1, 8, x.shape[-1]), axis=0)


def clip(x, lower, upper):
    return jnp.minimum(jnp.maximum(x, lower), upper)


def main_kernel(
    n,
    size,
    a_hbm,
    targets_hbm,
    lin_hbm,
    diag_hbm,
    lo_hbm,
    hi_hbm,
    mapped,
    alpha_ref,
    lower,
    upper,
    a_ref,
    at_ref,
    targets_ref,
    lin_ref,
    diag_ref,
    base_ref,
    lo_ref,
    hi_ref,
    step_ref,
    z_ref,
    u_ref,
    changes,
    acc,
    sums,
    terms,
    slots,
    sent,
    rounded,
    flat,
    running,
    mine,
    misfits,
    part,
    parts,
    grams,
    load_sem,
    send_a,
    recv_a,
    send_b,
    recv_b,
    send_c,
    recv_c,
):
    me = lax.axis_index("row")
    peers = peers_of(n, me)
    local = lin_ref.shape[0]
    k = a_ref.shape[0]

    loads = [
        pltpu.make_async_copy(source, target, load_sem.at[i])
        for i, (source, target) in enumerate(
            [
                (targets_hbm, targets_ref),
                (diag_hbm, diag_ref),
                (a_hbm, a_ref),
                (lo_hbm, lo_ref),
                (hi_hbm, hi_ref),
                (lin_hbm, lin_ref),
            ]
        )
    ]
    for load in loads:
        load.start()
    met = greet(n, peers)
    loads[0].wait()
    mine[...] = (0.0 - targets_ref[...]).astype(jnp.bfloat16)
    met()
    copies = start_spread(peers, me, mine, misfits, send_b, recv_b)

    loads[1].wait()
    lanes = diag_ref.shape[1]
    for i in range(diag_ref.shape[0]):
        line = 1.0 / (rho_plus_lip + diag_ref[i : i + 1, :])
        step_ref[i * lanes : (i + 1) * lanes, :] = jnp.broadcast_to(line, (lanes, lanes)).T
    loads[2].wait()

    def flip(at):
        at_ref[at, :] = a_ref[:, at].T

    chunks(local, size, flip)
    loads[3].wait()
    loads[4].wait()

    def bounds(at):
        lower[at, :] = lo_ref[at, :].astype(jnp.float32) * (1.0 / 64.0)
        upper[at, :] = hi_ref[at, :].astype(jnp.float32) * (1.0 / 64.0)

    chunks(local, size, bounds)
    loads[5].wait()
    acc[...] = jnp.zeros_like(acc)
    sums[...] = jnp.zeros_like(sums)
    half = me // (n // 2)

    def gradient_of(at, which):
        rows = pl.ds(pl.multiple_of(which * (n // 2), n // 2), n // 2)
        columns = pl.ds(pl.multiple_of(which * (k // 2), k // 2), k // 2)
        return jnp.dot(
            at_ref[at, columns],
            misfits[rows].reshape(k // 2, -1),
            preferred_element_type=jnp.float32,
        )

    def columns_of(which):
        return pl.ds(pl.multiple_of(which * (k // 2), k // 2), k // 2)

    def add_product(at, point):
        turned = point.astype(jnp.bfloat16).T
        flat[:, at] = turned
        columns = columns_of(1 - half)
        acc[:, columns] += jnp.dot(
            turned, at_ref[at, columns], preferred_element_type=jnp.float32
        )

    def send_terms(which, chosen):
        columns = columns_of(which)
        value = acc[:, columns].astype(terms.dtype)
        rounded[:, columns] = value
        rows = pl.ds(pl.multiple_of(which * (n // 2), n // 2), n // 2)
        terms[rows] = value.T.reshape((n // 2,) + terms.shape[1:])
        return [
            send(terms.at[peer], slots.at[d - 1], send_a.at[d], recv_a.at[d], peer)
            for d, peer in chosen
        ]

    def start_sum():
        copies = send_terms(1 - half, [peer for peer in peers if peer[0] >= n // 2])
        columns = columns_of(half)
        acc[:, columns] += jnp.dot(
            flat[...], at_ref[:, columns], preferred_element_type=jnp.float32
        )
        return copies + send_terms(half, [peer for peer in peers if peer[0] < n // 2])

    def near(at):
        base_ref[at, :] -= step_ref[at, :] * gradient_of(at, half)

    def gather_near(copies):
        for copy, (d, _) in zip(copies, peers):
            if d < n // 2:
                copy.wait_recv()
        chunks(local, size, near)
        for copy, (d, _) in zip(copies, peers):
            if d >= n // 2:
                copy.wait_recv()

    def raw_of(at):
        return base_ref[at, :] - step_ref[at, :] * gradient_of(at, 1 - half)

    def base(at):
        base_ref[at, :] = 0.0 - step_ref[at, :] * lin_ref[at, :]

    chunks(local, size, base)
    gather_near(copies)

    def start(at):
        raw = raw_of(at)
        boxed = clip(raw, lower[at, :], upper[at, :])
        scaled = raw - boxed
        mapped[0, 0, at, :] = boxed
        mapped[0, 1, at, :] = scaled
        sums[ITERS] += column_sum(boxed * boxed + scaled * scaled)
        add_product(at, boxed - scaled)

    chunks(local, size, start)
    for copy in copies:
        copy.wait_send()

    for iteration in range(1, ITERS):
        count = iteration + 1
        last = iteration == ITERS - 1
        copies = start_sum()
        if iteration == 1:
            sent[...] = rounded[...].astype(jnp.float32)
            total = terms[me].astype(jnp.float32) - targets_ref[...]
        else:
            sent[...] += rounded[...].astype(jnp.float32)
            total = terms[me].astype(jnp.float32) + running[...]
        acc[...] = 0.0 - sent[...]

        def state(at):
            if iteration == 1:
                return mapped[0, 0, at, :], mapped[0, 1, at, :]
            return z_ref[at, :], u_ref[at, :]

        def base(at):
            z, u = state(at)
            base_ref[at, :] = step_ref[at, :] * (rho_plus_lip * (z - u) - lin_ref[at, :]) + u

        chunks(local, size, base)
        for copy, (d, _) in reversed(list(zip(copies, peers))):
            copy.wait_recv()
            total = total + slots[d - 1].astype(jnp.float32)
        running[...] = total
        mine[...] = total.astype(jnp.bfloat16)
        spread = start_spread(peers, me, mine, misfits, send_b, recv_b)
        for copy in copies:
            copy.wait_send()
        gather_near(spread)

        def advance(at):
            z, u = state(at)
            raw = raw_of(at)
            boxed = clip(raw, lower[at, :], upper[at, :])
            scaled = raw - boxed
            mapped[iteration, 0, at, :] = boxed
            mapped[iteration, 1, at, :] = scaled
            cz, cu = boxed - z, scaled - u
            sums[0] += column_sum(cz * mapped[0, 0, at, :] + cu * mapped[0, 1, at, :])
            for i in range(1, iteration):
                sums[i] += column_sum(
                    cz * changes[i - 1, 0, at, :] + cu * changes[i - 1, 1, at, :]
                )
            sums[iteration] += column_sum(cz * cz + cu * cu)

        pieces(local, min(512, local), advance)
        for copy in spread:
            copy.wait_send()

        kept = list(range(count)) + ([ITERS] if iteration == 1 else [])
        for i in kept:
            row = i if i < ITERS else ITERS - 1
            part[row : row + 1, :] = jnp.sum(sums[i], axis=0, keepdims=True)
        spread = start_spread(peers, me, part, parts, send_c, recv_c)
        sums[...] = jnp.zeros_like(sums)

        def keep(at):
            for j, before in enumerate(state(at)):
                changes[iteration - 1, j, at, :] = mapped[iteration, j, at, :] - before

        if not last:
            chunks(local, size, keep)
        finish(spread)
        whole = parts[0]
        for i in range(1, n):
            whole = whole + parts[i]
        grams[iteration - 1] = whole

        gram = [[None] * count for _ in range(count)]
        gram[0][0] = grams[0, ITERS - 1 : ITERS, :]
        for i in range(1, count):
            for j in range(i + 1):
                gram[i][j] = gram[j][i] = grams[i - 1, j : j + 1, :]
        for i, row in enumerate(mix_weights(gram)):
            alpha_ref[i : i + 1, :] = row

        if last:
            break

        def mix(at):
            z = alpha_ref[0:1, :] * mapped[0, 0, at, :]
            u = alpha_ref[0:1, :] * mapped[0, 1, at, :]
            for i in range(1, count):
                z = z + alpha_ref[i : i + 1, :] * mapped[i, 0, at, :]
                u = u + alpha_ref[i : i + 1, :] * mapped[i, 1, at, :]
            z = clip(z, lower[at, :], upper[at, :])
            z_ref[at, :] = z
            u_ref[at, :] = u
            add_product(at, z - u)

        pieces(local, min(512, local), mix)


def mix_kernel(size, mapped, alpha_ref, lower, upper, z_hbm, u_hbm, z_ref, u_ref, sem):
    local = lower.shape[0]
    steps = local // size
    copies = []
    for step in range(steps):
        at = pl.ds(step * size, size)
        z = alpha_ref[0:1, :] * mapped[0, 0, at, :]
        u = alpha_ref[0:1, :] * mapped[0, 1, at, :]
        for i in range(1, ITERS):
            z = z + alpha_ref[i : i + 1, :] * mapped[i, 0, at, :]
            u = u + alpha_ref[i : i + 1, :] * mapped[i, 1, at, :]
        z_ref[at, :] = clip(z, lower[at, :], upper[at, :])
        u_ref[at, :] = u
        for j, (src, dst) in enumerate([(z_ref, z_hbm), (u_ref, u_hbm)]):
            copy = pltpu.make_async_copy(src.at[at, :], dst.at[at, :], sem.at[j, step])
            copy.start()
            copies.append(copy)
    for copy in copies:
        copy.wait()


def per_device(n, design_matrix, targets, linear, diagonal, lower_code, upper_code):
    k = design_matrix.shape[0]
    local, s = linear.shape
    kr = k // n
    size = min(2048, local)
    big = (local, s)
    lines = diagonal.reshape(local // s, s)
    vmem = pl.BlockSpec(memory_space=pltpu.VMEM)
    hbm = pl.BlockSpec(memory_space=pl.ANY)
    dma = pltpu.SemaphoreType.DMA((n,))
    mapped, alpha, lower, upper = pl.pallas_call(
        functools.partial(main_kernel, n, size),
        in_specs=[hbm] * 6,
        out_specs=[vmem] * 4,
        out_shape=[
            pltpu.VMEM((ITERS, 2, local, s), jnp.float32),
            pltpu.VMEM((8, s), jnp.float32),
            pltpu.VMEM(big, jnp.float32),
            pltpu.VMEM(big, jnp.float32),
        ],
        scratch_shapes=[
            pltpu.VMEM((k, local), jnp.bfloat16),
            pltpu.VMEM((local, k), jnp.bfloat16),
            pltpu.VMEM((kr, s), jnp.float32),
            pltpu.VMEM(big, jnp.float32),
            pltpu.VMEM((local // s, s), jnp.float32),
            pltpu.VMEM(big, jnp.float32),
            pltpu.VMEM(big, jnp.int32),
            pltpu.VMEM(big, jnp.int32),
            pltpu.VMEM(big, jnp.float32),
            pltpu.VMEM(big, jnp.float32),
            pltpu.VMEM(big, jnp.float32),
            pltpu.VMEM((ITERS - 2, 2, local, s), jnp.float32),
            pltpu.VMEM((s, k), jnp.float32),
            pltpu.VMEM((ITERS + 1, 8, s), jnp.float32),
            pltpu.VMEM((n, kr, s), TERM),
            pltpu.VMEM((n - 1, kr, s), TERM),
            pltpu.VMEM((s, k), jnp.float32),
            pltpu.VMEM((s, k), TERM),
            pltpu.VMEM((s, local), jnp.bfloat16),
            pltpu.VMEM((kr, s), jnp.float32),
            pltpu.VMEM((kr, s), jnp.bfloat16),
            pltpu.VMEM((n, kr, s), jnp.bfloat16),
            pltpu.VMEM((ITERS, s), jnp.float32),
            pltpu.VMEM((n, ITERS, s), jnp.float32),
            pltpu.VMEM((ITERS - 1, ITERS, s), jnp.float32),
            pltpu.SemaphoreType.DMA((6,)),
        ]
        + [dma] * 6,
        compiler_params=pltpu.CompilerParams(
            collective_id=0, has_side_effects=True, vmem_limit_bytes=40 * 1024 * 1024
        ),
        name="main",
    )(design_matrix, targets, linear, lines, lower_code, upper_code)
    return pl.pallas_call(
        functools.partial(mix_kernel, min(512, local)),
        in_specs=[vmem] * 4,
        out_specs=[hbm] * 2,
        out_shape=[jax.ShapeDtypeStruct(big, jnp.float32)] * 2,
        scratch_shapes=[
            pltpu.VMEM(big, jnp.float32),
            pltpu.VMEM(big, jnp.float32),
            pltpu.SemaphoreType.DMA((2, local // min(512, local))),
        ],
        compiler_params=pltpu.CompilerParams(vmem_limit_bytes=8 * 1024 * 1024),
        name="last_mix",
    )(mapped, alpha, lower, upper)


def solution(mesh):
    in_specs = (
        P("groups", "row"),
        P(("groups", "row"), None),
        P(("groups", "row"), None),
        P(("groups", "row")),
        P(("groups", "row"), None),
        P(("groups", "row"), None),
    )
    out_specs = (P(("groups", "row"), None), P(("groups", "row"), None))
    return jax.shard_map(
        functools.partial(per_device, mesh.shape["row"]),
        mesh=mesh,
        in_specs=in_specs,
        out_specs=out_specs,
        check_vma=False,
    )
```

```python
import functools

import jax
import jax.numpy as jnp
from jax import lax
from jax.experimental import pallas as pl
from jax.experimental.pallas import tpu as pltpu
from jax.sharding import PartitionSpec as P

ITERS = 4
TERM = jnp.bfloat16

rho_plus_lip = 7.0


def solve_small(matrix, rhs):
    count = len(rhs)
    table = [list(line) for line in matrix]
    right = list(rhs)
    inverse = []
    for p in range(count):
        inverse.append(1.0 / table[p][p])
        for i in range(p + 1, count):
            factor = table[i][p] * inverse[p]
            for j in range(p + 1, count):
                table[i][j] = table[i][j] - factor * table[p][j]
            right[i] = right[i] - factor * right[p]
    result = [None] * count
    for i in reversed(range(count)):
        total = right[i]
        for j in range(i + 1, count):
            total = total - table[i][j] * result[j]
        result[i] = total * inverse[i]
    return result


def mix_weights(gram):
    count = len(gram)
    trace = gram[0][0]
    for i in range(1, count):
        trace = trace + gram[i][i]
    shift = 0.01 * trace / count + 1e-06
    matrix = [[gram[i][j] + (shift if i == j else 0.0) for j in range(count)] for i in range(count)]
    solved = solve_small(matrix, [jnp.ones_like(trace)] * count)
    total = solved[0]
    for i in range(1, count):
        total = total + solved[i]
    scale = 1.0 / total
    return [item * scale for item in solved]


def peers_of(n, me):
    found = []
    for d in range(n - 1, 0, -1):
        peer = me
        bit = 1
        while bit < n:
            if d & bit:
                peer = peer + bit * (1 - 2 * ((me // bit) % 2))
            bit *= 2
        found.append((d, peer))
    return found


def greet(n, peers):
    barrier = pltpu.get_barrier_semaphore()
    for _, peer in peers:
        pl.semaphore_signal(
            barrier,
            inc=1,
            device_id={"row": peer},
            device_id_type=pl.DeviceIdType.MESH,
        )
    return lambda: pl.semaphore_wait(barrier, n - 1)


def send(src, dst, send_sem, recv_sem, peer):
    copy = pltpu.make_async_remote_copy(
        src_ref=src,
        dst_ref=dst,
        send_sem=send_sem,
        recv_sem=recv_sem,
        device_id={"row": peer},
        device_id_type=pl.DeviceIdType.MESH,
    )
    copy.start()
    return copy


def start_spread(peers, me, mine, whole, send_sem, recv_sem):
    copies = [
        send(mine, whole.at[me], send_sem.at[d], recv_sem.at[d], peer) for d, peer in peers
    ]
    whole[me] = mine[...]
    return copies


def chunks(local, size, body):
    def step(i, carry):
        body(pl.ds(pl.multiple_of(i * size, size), size))
        return carry

    lax.fori_loop(0, local // size, step, 0)


def pieces(local, size, body):
    for i in range(local // size):
        body(pl.ds(i * size, size))


def column_sum(x):
    return jnp.sum(x.reshape(-1, 8, x.shape[-1]), axis=0)


def clip(x, lower, upper):
    return jnp.minimum(jnp.maximum(x, lower), upper)


def main_kernel(
    n,
    size,
    a_hbm,
    targets_hbm,
    lin_hbm,
    diag_hbm,
    lo_hbm,
    hi_hbm,
    mapped,
    alpha_ref,
    lower,
    upper,
    a_ref,
    at_ref,
    targets_ref,
    lin_ref,
    diag_ref,
    base_ref,
    lo_ref,
    hi_ref,
    step_ref,
    z_ref,
    u_ref,
    changes,
    acc,
    sums,
    terms,
    slots,
    sent,
    rounded,
    flat,
    running,
    mine,
    misfits,
    part,
    parts,
    grams,
    load_sem,
    send_a,
    recv_a,
    send_b,
    recv_b,
    send_c,
    recv_c,
):
    me = lax.axis_index("row")
    peers = peers_of(n, me)
    local = lin_ref.shape[0]
    k = a_ref.shape[0]

    loads = [
        pltpu.make_async_copy(source, target, load_sem.at[i])
        for i, (source, target) in enumerate(
            [
                (targets_hbm, targets_ref),
                (diag_hbm, diag_ref),
                (a_hbm, a_ref),
                (lo_hbm, lo_ref),
                (hi_hbm, hi_ref),
                (lin_hbm, lin_ref),
            ]
        )
    ]
    for load in loads:
        load.start()
    met = greet(n, peers)
    loads[0].wait()
    mine[...] = (0.0 - targets_ref[...]).astype(jnp.bfloat16)
    met()
    copies = start_spread(peers, me, mine, misfits, send_b, recv_b)

    loads[1].wait()
    lanes = diag_ref.shape[1]
    for i in range(diag_ref.shape[0]):
        line = 1.0 / (rho_plus_lip + diag_ref[i : i + 1, :])
        step_ref[i * lanes : (i + 1) * lanes, :] = jnp.broadcast_to(line, (lanes, lanes)).T
    loads[2].wait()

    def flip(at):
        at_ref[at, :] = a_ref[:, at].T

    chunks(local, size, flip)
    loads[3].wait()
    loads[4].wait()

    def bounds(at):
        lower[at, :] = lo_ref[at, :].astype(jnp.float32) * (1.0 / 64.0)
        upper[at, :] = hi_ref[at, :].astype(jnp.float32) * (1.0 / 64.0)

    chunks(local, size, bounds)
    loads[5].wait()
    acc[...] = jnp.zeros_like(acc)
    sums[...] = jnp.zeros_like(sums)
    half = me // (n // 2)

    def gradient_of(at, which):
        rows = pl.ds(pl.multiple_of(which * (n // 2), n // 2), n // 2)
        columns = pl.ds(pl.multiple_of(which * (k // 2), k // 2), k // 2)
        return jnp.dot(
            at_ref[at, columns],
            misfits[rows].reshape(k // 2, -1),
            preferred_element_type=jnp.float32,
        )

    def columns_of(which):
        return pl.ds(pl.multiple_of(which * (k // 2), k // 2), k // 2)

    def add_product(at, point):
        turned = point.astype(jnp.bfloat16).T
        flat[:, at] = turned
        columns = columns_of(1 - half)
        acc[:, columns] += jnp.dot(
            turned, at_ref[at, columns], preferred_element_type=jnp.float32
        )

    def send_terms(which, chosen):
        columns = columns_of(which)
        value = acc[:, columns].astype(terms.dtype)
        rounded[:, columns] = value
        rows = pl.ds(pl.multiple_of(which * (n // 2), n // 2), n // 2)
        terms[rows] = value.T.reshape((n // 2,) + terms.shape[1:])
        return [
            send(terms.at[peer], slots.at[d - 1], send_a.at[d], recv_a.at[d], peer)
            for d, peer in chosen
        ]

    def start_sum():
        copies = send_terms(1 - half, [peer for peer in peers if peer[0] >= n // 2])
        columns = columns_of(half)
        acc[:, columns] += jnp.dot(
            flat[...], at_ref[:, columns], preferred_element_type=jnp.float32
        )
        return copies + send_terms(half, [peer for peer in peers if peer[0] < n // 2])

    def near(at):
        base_ref[at, :] -= step_ref[at, :] * gradient_of(at, half)

    def gather_near(copies):
        for copy, (d, _) in zip(copies, peers):
            if d < n // 2:
                copy.wait_recv()
        chunks(local, size, near)
        for copy, (d, _) in zip(copies, peers):
            if d >= n // 2:
                copy.wait_recv()

    def raw_of(at):
        return base_ref[at, :] - step_ref[at, :] * gradient_of(at, 1 - half)

    def base(at):
        base_ref[at, :] = 0.0 - step_ref[at, :] * lin_ref[at, :]

    chunks(local, size, base)
    gather_near(copies)

    def start(at):
        raw = raw_of(at)
        boxed = clip(raw, lower[at, :], upper[at, :])
        scaled = raw - boxed
        mapped[0, 0, at, :] = boxed
        mapped[0, 1, at, :] = scaled
        sums[ITERS] += column_sum(boxed * boxed + scaled * scaled)
        add_product(at, boxed - scaled)

    pieces(local, min(1024, local), start)
    spread = copies

    for iteration in range(1, ITERS):
        count = iteration + 1
        last = iteration == ITERS - 1
        copies = start_sum()
        for copy in spread if iteration == 1 else held:
            copy.wait_send()
        if iteration == 1:
            sent[...] = rounded[...].astype(jnp.float32)
            total = terms[me].astype(jnp.float32) - targets_ref[...]
        else:
            sent[...] += rounded[...].astype(jnp.float32)
            total = terms[me].astype(jnp.float32) + running[...]
        acc[...] = 0.0 - sent[...]

        def state(at):
            if iteration == 1:
                return mapped[0, 0, at, :], mapped[0, 1, at, :]
            return z_ref[at, :], u_ref[at, :]

        def base(at):
            z, u = state(at)
            base_ref[at, :] = step_ref[at, :] * (rho_plus_lip * (z - u) - lin_ref[at, :]) + u

        chunks(local, size, base)
        for copy, (d, _) in reversed(list(zip(copies, peers))):
            copy.wait_recv()
            total = total + slots[d - 1].astype(jnp.float32)
        running[...] = total
        mine[...] = total.astype(jnp.bfloat16)
        spread = start_spread(peers, me, mine, misfits, send_b, recv_b)
        for copy in copies:
            copy.wait_send()
        gather_near(spread)

        def advance(at):
            z, u = state(at)
            raw = raw_of(at)
            boxed = clip(raw, lower[at, :], upper[at, :])
            scaled = raw - boxed
            mapped[iteration, 0, at, :] = boxed
            mapped[iteration, 1, at, :] = scaled
            cz, cu = boxed - z, scaled - u
            sums[0] += column_sum(cz * mapped[0, 0, at, :] + cu * mapped[0, 1, at, :])
            for i in range(1, iteration):
                sums[i] += column_sum(
                    cz * changes[i - 1, 0, at, :] + cu * changes[i - 1, 1, at, :]
                )
            sums[iteration] += column_sum(cz * cz + cu * cu)

        pieces(local, min(512, local), advance)
        gathered = spread

        kept = list(range(count)) + ([ITERS] if iteration == 1 else [])
        for i in kept:
            row = i if i < ITERS else ITERS - 1
            part[row : row + 1, :] = jnp.sum(sums[i], axis=0, keepdims=True)
        spread = start_spread(peers, me, part, parts, send_c, recv_c)
        for copy in gathered:
            copy.wait_send()
        sums[...] = jnp.zeros_like(sums)

        def keep(at):
            for j, before in enumerate(state(at)):
                changes[iteration - 1, j, at, :] = mapped[iteration, j, at, :] - before

        if not last:
            chunks(local, size, keep)
        for copy in reversed(spread):
            copy.wait_recv()
        whole = parts[0]
        for i in range(1, n):
            whole = whole + parts[i]
        grams[iteration - 1] = whole

        gram = [[None] * count for _ in range(count)]
        gram[0][0] = grams[0, ITERS - 1 : ITERS, :]
        for i in range(1, count):
            for j in range(i + 1):
                gram[i][j] = gram[j][i] = grams[i - 1, j : j + 1, :]
        for i, row in enumerate(mix_weights(gram)):
            alpha_ref[i : i + 1, :] = row

        if last:
            for copy in spread:
                copy.wait_send()
            break

        def mix(at):
            z = alpha_ref[0:1, :] * mapped[0, 0, at, :]
            u = alpha_ref[0:1, :] * mapped[0, 1, at, :]
            for i in range(1, count):
                z = z + alpha_ref[i : i + 1, :] * mapped[i, 0, at, :]
                u = u + alpha_ref[i : i + 1, :] * mapped[i, 1, at, :]
            z = clip(z, lower[at, :], upper[at, :])
            z_ref[at, :] = z
            u_ref[at, :] = u
            add_product(at, z - u)

        pieces(local, min(512, local), mix)
        held = spread


def mix_kernel(size, mapped, alpha_ref, lower, upper, z_hbm, u_hbm, z_ref, u_ref, sem):
    local = lower.shape[0]
    steps = local // size
    copies = []
    for step in range(steps):
        at = pl.ds(step * size, size)
        z = alpha_ref[0:1, :] * mapped[0, 0, at, :]
        u = alpha_ref[0:1, :] * mapped[0, 1, at, :]
        for i in range(1, ITERS):
            z = z + alpha_ref[i : i + 1, :] * mapped[i, 0, at, :]
            u = u + alpha_ref[i : i + 1, :] * mapped[i, 1, at, :]
        z_ref[at, :] = clip(z, lower[at, :], upper[at, :])
        u_ref[at, :] = u
        for j, (src, dst) in enumerate([(z_ref, z_hbm), (u_ref, u_hbm)]):
            copy = pltpu.make_async_copy(src.at[at, :], dst.at[at, :], sem.at[j, step])
            copy.start()
            copies.append(copy)
    for copy in copies:
        copy.wait()


def per_device(n, design_matrix, targets, linear, diagonal, lower_code, upper_code):
    k = design_matrix.shape[0]
    local, s = linear.shape
    kr = k // n
    size = min(2048, local)
    big = (local, s)
    lines = diagonal.reshape(local // s, s)
    vmem = pl.BlockSpec(memory_space=pltpu.VMEM)
    hbm = pl.BlockSpec(memory_space=pl.ANY)
    dma = pltpu.SemaphoreType.DMA((n,))
    mapped, alpha, lower, upper = pl.pallas_call(
        functools.partial(main_kernel, n, size),
        in_specs=[hbm] * 6,
        out_specs=[vmem] * 4,
        out_shape=[
            pltpu.VMEM((ITERS, 2, local, s), jnp.float32),
            pltpu.VMEM((8, s), jnp.float32),
            pltpu.VMEM(big, jnp.float32),
            pltpu.VMEM(big, jnp.float32),
        ],
        scratch_shapes=[
            pltpu.VMEM((k, local), jnp.bfloat16),
            pltpu.VMEM((local, k), jnp.bfloat16),
            pltpu.VMEM((kr, s), jnp.float32),
            pltpu.VMEM(big, jnp.float32),
            pltpu.VMEM((local // s, s), jnp.float32),
            pltpu.VMEM(big, jnp.float32),
            pltpu.VMEM(big, jnp.int32),
            pltpu.VMEM(big, jnp.int32),
            pltpu.VMEM(big, jnp.float32),
            pltpu.VMEM(big, jnp.float32),
            pltpu.VMEM(big, jnp.float32),
            pltpu.VMEM((ITERS - 2, 2, local, s), jnp.float32),
            pltpu.VMEM((s, k), jnp.float32),
            pltpu.VMEM((ITERS + 1, 8, s), jnp.float32),
            pltpu.VMEM((n, kr, s), TERM),
            pltpu.VMEM((n - 1, kr, s), TERM),
            pltpu.VMEM((s, k), jnp.float32),
            pltpu.VMEM((s, k), TERM),
            pltpu.VMEM((s, local), jnp.bfloat16),
            pltpu.VMEM((kr, s), jnp.float32),
            pltpu.VMEM((kr, s), jnp.bfloat16),
            pltpu.VMEM((n, kr, s), jnp.bfloat16),
            pltpu.VMEM((ITERS, s), jnp.float32),
            pltpu.VMEM((n, ITERS, s), jnp.float32),
            pltpu.VMEM((ITERS - 1, ITERS, s), jnp.float32),
            pltpu.SemaphoreType.DMA((6,)),
        ]
        + [dma] * 6,
        compiler_params=pltpu.CompilerParams(
            collective_id=0, has_side_effects=True, vmem_limit_bytes=40 * 1024 * 1024
        ),
        name="main",
    )(design_matrix, targets, linear, lines, lower_code, upper_code)
    return pl.pallas_call(
        functools.partial(mix_kernel, min(512, local)),
        in_specs=[vmem] * 4,
        out_specs=[hbm] * 2,
        out_shape=[jax.ShapeDtypeStruct(big, jnp.float32)] * 2,
        scratch_shapes=[
            pltpu.VMEM(big, jnp.float32),
            pltpu.VMEM(big, jnp.float32),
            pltpu.SemaphoreType.DMA((2, local // min(512, local))),
        ],
        compiler_params=pltpu.CompilerParams(vmem_limit_bytes=8 * 1024 * 1024),
        name="last_mix",
    )(mapped, alpha, lower, upper)


def solution(mesh):
    in_specs = (
        P("groups", "row"),
        P(("groups", "row"), None),
        P(("groups", "row"), None),
        P(("groups", "row")),
        P(("groups", "row"), None),
        P(("groups", "row"), None),
    )
    out_specs = (P(("groups", "row"), None), P(("groups", "row"), None))
    return jax.shard_map(
        functools.partial(per_device, mesh.shape["row"]),
        mesh=mesh,
        in_specs=in_specs,
        out_specs=out_specs,
        check_vma=False,
    )
```

```python
import functools

import jax
import jax.numpy as jnp
from jax import lax
from jax.experimental import pallas as pl
from jax.experimental.pallas import tpu as pltpu
from jax.sharding import PartitionSpec as P

ITERS = 4
TERM = jnp.bfloat16

rho_plus_lip = 7.0


def solve_small(matrix, rhs):
    count = len(rhs)
    table = [list(line) for line in matrix]
    right = list(rhs)
    inverse = []
    for p in range(count):
        inverse.append(1.0 / table[p][p])
        for i in range(p + 1, count):
            factor = table[i][p] * inverse[p]
            for j in range(p + 1, count):
                table[i][j] = table[i][j] - factor * table[p][j]
            right[i] = right[i] - factor * right[p]
    result = [None] * count
    for i in reversed(range(count)):
        total = right[i]
        for j in range(i + 1, count):
            total = total - table[i][j] * result[j]
        result[i] = total * inverse[i]
    return result


def mix_weights(gram):
    count = len(gram)
    trace = gram[0][0]
    for i in range(1, count):
        trace = trace + gram[i][i]
    shift = 0.01 * trace / count + 1e-06
    matrix = [[gram[i][j] + (shift if i == j else 0.0) for j in range(count)] for i in range(count)]
    solved = solve_small(matrix, [jnp.ones_like(trace)] * count)
    total = solved[0]
    for i in range(1, count):
        total = total + solved[i]
    scale = 1.0 / total
    return [item * scale for item in solved]


def peers_of(n, me):
    found = []
    for d in range(n - 1, 0, -1):
        peer = me
        bit = 1
        while bit < n:
            if d & bit:
                peer = peer + bit * (1 - 2 * ((me // bit) % 2))
            bit *= 2
        found.append((d, peer))
    return found


def greet(n, peers):
    barrier = pltpu.get_barrier_semaphore()
    for _, peer in peers:
        pl.semaphore_signal(
            barrier,
            inc=1,
            device_id={"row": peer},
            device_id_type=pl.DeviceIdType.MESH,
        )
    return lambda: pl.semaphore_wait(barrier, n - 1)


def send(src, dst, send_sem, recv_sem, peer):
    copy = pltpu.make_async_remote_copy(
        src_ref=src,
        dst_ref=dst,
        send_sem=send_sem,
        recv_sem=recv_sem,
        device_id={"row": peer},
        device_id_type=pl.DeviceIdType.MESH,
    )
    copy.start()
    return copy


def start_spread(peers, me, mine, whole, send_sem, recv_sem):
    copies = [
        send(mine, whole.at[me], send_sem.at[d], recv_sem.at[d], peer) for d, peer in peers
    ]
    whole[me] = mine[...]
    return copies


def chunks(local, size, body):
    def step(i, carry):
        body(pl.ds(pl.multiple_of(i * size, size), size))
        return carry

    lax.fori_loop(0, local // size, step, 0)


def pieces(local, size, body):
    for i in range(local // size):
        body(pl.ds(i * size, size))


def column_sum(x):
    return jnp.sum(x.reshape(-1, 8, x.shape[-1]), axis=0)


def clip(x, lower, upper):
    return jnp.minimum(jnp.maximum(x, lower), upper)


def main_kernel(
    n,
    size,
    a_hbm,
    targets_hbm,
    lin_hbm,
    diag_hbm,
    lo_hbm,
    hi_hbm,
    mapped,
    alpha_ref,
    lower,
    upper,
    a_ref,
    at_ref,
    targets_ref,
    lin_ref,
    diag_ref,
    base_ref,
    low_ref,
    high_ref,
    lo_ref,
    hi_ref,
    step_ref,
    z_ref,
    u_ref,
    changes,
    acc,
    sums,
    terms,
    slots,
    sent,
    rounded,
    flat,
    running,
    mine,
    misfits,
    part,
    parts,
    grams,
    load_sem,
    send_a,
    recv_a,
    send_b,
    recv_b,
    send_c,
    recv_c,
):
    me = lax.axis_index("row")
    peers = peers_of(n, me)
    local = lin_ref.shape[0]
    k = a_ref.shape[0]

    loads = [
        pltpu.make_async_copy(source, target, load_sem.at[i])
        for i, (source, target) in enumerate(
            [
                (targets_hbm, targets_ref),
                (diag_hbm, diag_ref),
                (a_hbm, a_ref),
                (lo_hbm, lo_ref),
                (hi_hbm, hi_ref),
                (lin_hbm, lin_ref),
            ]
        )
    ]
    for load in loads:
        load.start()
    met = greet(n, peers)
    loads[0].wait()
    mine[...] = (0.0 - targets_ref[...]).astype(jnp.bfloat16)
    met()
    copies = start_spread(peers, me, mine, misfits, send_b, recv_b)

    loads[1].wait()
    lanes = diag_ref.shape[1]
    for i in range(diag_ref.shape[0]):
        line = 1.0 / (rho_plus_lip + diag_ref[i : i + 1, :])
        step_ref[i * lanes : (i + 1) * lanes, :] = jnp.broadcast_to(line, (lanes, lanes)).T
    loads[2].wait()

    def flip(at):
        at_ref[at, :] = a_ref[:, at].T

    chunks(local, size, flip)
    loads[3].wait()
    loads[4].wait()

    def bounds(at):
        lower[at, :] = lo_ref[at, :].astype(jnp.float32) * (1.0 / 64.0)
        upper[at, :] = hi_ref[at, :].astype(jnp.float32) * (1.0 / 64.0)

    chunks(local, size, bounds)
    loads[5].wait()
    acc[...] = jnp.zeros_like(acc)
    sums[...] = jnp.zeros_like(sums)
    half = me // (n // 2)

    def gradient_of(at, which):
        rows = pl.ds(pl.multiple_of(which * (n // 2), n // 2), n // 2)
        columns = pl.ds(pl.multiple_of(which * (k // 2), k // 2), k // 2)
        return jnp.dot(
            at_ref[at, columns],
            misfits[rows].reshape(k // 2, -1),
            preferred_element_type=jnp.float32,
        )

    def columns_of(which):
        return pl.ds(pl.multiple_of(which * (k // 2), k // 2), k // 2)

    def add_product(at, point):
        turned = point.astype(jnp.bfloat16).T
        flat[:, at] = turned
        columns = columns_of(1 - half)
        acc[:, columns] += jnp.dot(
            turned, at_ref[at, columns], preferred_element_type=jnp.float32
        )

    def send_terms(which, chosen):
        columns = columns_of(which)
        value = acc[:, columns].astype(terms.dtype)
        rounded[:, columns] = value
        rows = pl.ds(pl.multiple_of(which * (n // 2), n // 2), n // 2)
        terms[rows] = value.T.reshape((n // 2,) + terms.shape[1:])
        return [
            send(terms.at[peer], slots.at[d - 1], send_a.at[d], recv_a.at[d], peer)
            for d, peer in chosen
        ]

    def start_sum():
        copies = send_terms(1 - half, [peer for peer in peers if peer[0] >= n // 2])
        columns = columns_of(half)
        acc[:, columns] += jnp.dot(
            flat[...], at_ref[:, columns], preferred_element_type=jnp.float32
        )
        return copies + send_terms(half, [peer for peer in peers if peer[0] < n // 2])

    def near(at):
        base_ref[at, :] -= step_ref[at, :] * gradient_of(at, half)

    def gather_near(copies):
        for copy, (d, _) in zip(copies, peers):
            if d < n // 2:
                copy.wait_recv()
        chunks(local, size, near)
        for copy, (d, _) in zip(copies, peers):
            if d >= n // 2:
                copy.wait_recv()

    def raw_of(at):
        return base_ref[at, :] - step_ref[at, :] * gradient_of(at, 1 - half)

    def base(at):
        base_ref[at, :] = 0.0 - step_ref[at, :] * lin_ref[at, :]

    chunks(local, size, base)
    gather_near(copies)

    def start(at):
        raw = raw_of(at)
        boxed = clip(raw, lower[at, :], upper[at, :])
        scaled = raw - boxed
        mapped[0, 0, at, :] = boxed
        mapped[0, 1, at, :] = scaled
        sums[ITERS] += column_sum(boxed * boxed + scaled * scaled)
        add_product(at, boxed - scaled)

    pieces(local, min(1024, local), start)
    spread = copies

    for iteration in range(1, ITERS):
        count = iteration + 1
        last = iteration == ITERS - 1
        copies = start_sum()
        for copy in spread if iteration == 1 else held:
            copy.wait_send()
        if iteration == 1:
            sent[...] = rounded[...].astype(jnp.float32)
            total = terms[me].astype(jnp.float32) - targets_ref[...]
        else:
            sent[...] += rounded[...].astype(jnp.float32)
            total = terms[me].astype(jnp.float32) + running[...]
        acc[...] = 0.0 - sent[...]

        def state(at):
            if iteration == 1:
                return mapped[0, 0, at, :], mapped[0, 1, at, :]
            return z_ref[at, :], u_ref[at, :]

        def base(at):
            z, u = state(at)
            step = step_ref[at, :]
            base_ref[at, :] = step * (rho_plus_lip * (z - u) - lin_ref[at, :]) + (u - z)
            low_ref[at, :] = lower[at, :] - z
            high_ref[at, :] = upper[at, :] - z

        chunks(local, size, base)
        for copy, (d, _) in reversed(list(zip(copies, peers))):
            copy.wait_recv()
            total = total + slots[d - 1].astype(jnp.float32)
        running[...] = total
        mine[...] = total.astype(jnp.bfloat16)
        spread = start_spread(peers, me, mine, misfits, send_b, recv_b)
        for copy in copies:
            copy.wait_send()
        gather_near(spread)

        def advance(at):
            shifted = raw_of(at)
            cz = clip(shifted, low_ref[at, :], high_ref[at, :])
            cu = shifted - cz - state(at)[1]
            if last:
                mapped[iteration, 0, at, :] = cz
                mapped[iteration, 1, at, :] = cu
            else:
                changes[iteration - 1, 0, at, :] = cz
                changes[iteration - 1, 1, at, :] = cu
            sums[0] += column_sum(cz * mapped[0, 0, at, :] + cu * mapped[0, 1, at, :])
            for i in range(1, iteration):
                sums[i] += column_sum(
                    cz * changes[i - 1, 0, at, :] + cu * changes[i - 1, 1, at, :]
                )
            sums[iteration] += column_sum(cz * cz + cu * cu)

        pieces(local, min(512, local), advance)
        gathered = spread

        kept = list(range(count)) + ([ITERS] if iteration == 1 else [])
        for i in kept:
            row = i if i < ITERS else ITERS - 1
            part[row : row + 1, :] = jnp.sum(sums[i], axis=0, keepdims=True)
        spread = start_spread(peers, me, part, parts, send_c, recv_c)
        for copy in gathered:
            copy.wait_send()
        sums[...] = jnp.zeros_like(sums)

        def keep(at):
            for j, before in enumerate(state(at)):
                change = mapped[iteration, j, at, :] if last else changes[iteration - 1, j, at, :]
                mapped[iteration, j, at, :] = before + change

        chunks(local, size, keep)
        for copy in reversed(spread):
            copy.wait_recv()
        whole = parts[0]
        for i in range(1, n):
            whole = whole + parts[i]
        grams[iteration - 1] = whole

        gram = [[None] * count for _ in range(count)]
        gram[0][0] = grams[0, ITERS - 1 : ITERS, :]
        for i in range(1, count):
            for j in range(i + 1):
                gram[i][j] = gram[j][i] = grams[i - 1, j : j + 1, :]
        for i, row in enumerate(mix_weights(gram)):
            alpha_ref[i : i + 1, :] = row

        if last:
            for copy in spread:
                copy.wait_send()
            break

        def mix(at):
            z = alpha_ref[0:1, :] * mapped[0, 0, at, :]
            u = alpha_ref[0:1, :] * mapped[0, 1, at, :]
            for i in range(1, count):
                z = z + alpha_ref[i : i + 1, :] * mapped[i, 0, at, :]
                u = u + alpha_ref[i : i + 1, :] * mapped[i, 1, at, :]
            z = clip(z, lower[at, :], upper[at, :])
            z_ref[at, :] = z
            u_ref[at, :] = u
            add_product(at, z - u)

        pieces(local, min(512, local), mix)
        held = spread


def mix_kernel(size, mapped, alpha_ref, lower, upper, z_hbm, u_hbm, z_ref, u_ref, sem):
    local = lower.shape[0]
    steps = local // size
    copies = []
    for step in range(steps):
        at = pl.ds(step * size, size)
        z = alpha_ref[0:1, :] * mapped[0, 0, at, :]
        u = alpha_ref[0:1, :] * mapped[0, 1, at, :]
        for i in range(1, ITERS):
            z = z + alpha_ref[i : i + 1, :] * mapped[i, 0, at, :]
            u = u + alpha_ref[i : i + 1, :] * mapped[i, 1, at, :]
        z_ref[at, :] = clip(z, lower[at, :], upper[at, :])
        u_ref[at, :] = u
        for j, (src, dst) in enumerate([(z_ref, z_hbm), (u_ref, u_hbm)]):
            copy = pltpu.make_async_copy(src.at[at, :], dst.at[at, :], sem.at[j, step])
            copy.start()
            copies.append(copy)
    for copy in copies:
        copy.wait()


def per_device(n, design_matrix, targets, linear, diagonal, lower_code, upper_code):
    k = design_matrix.shape[0]
    local, s = linear.shape
    kr = k // n
    size = min(2048, local)
    big = (local, s)
    lines = diagonal.reshape(local // s, s)
    vmem = pl.BlockSpec(memory_space=pltpu.VMEM)
    hbm = pl.BlockSpec(memory_space=pl.ANY)
    dma = pltpu.SemaphoreType.DMA((n,))
    mapped, alpha, lower, upper = pl.pallas_call(
        functools.partial(main_kernel, n, size),
        in_specs=[hbm] * 6,
        out_specs=[vmem] * 4,
        out_shape=[
            pltpu.VMEM((ITERS, 2, local, s), jnp.float32),
            pltpu.VMEM((8, s), jnp.float32),
            pltpu.VMEM(big, jnp.float32),
            pltpu.VMEM(big, jnp.float32),
        ],
        scratch_shapes=[
            pltpu.VMEM((k, local), jnp.bfloat16),
            pltpu.VMEM((local, k), jnp.bfloat16),
            pltpu.VMEM((kr, s), jnp.float32),
            pltpu.VMEM(big, jnp.float32),
            pltpu.VMEM((local // s, s), jnp.float32),
            pltpu.VMEM(big, jnp.float32),
            pltpu.VMEM(big, jnp.float32),
            pltpu.VMEM(big, jnp.float32),
            pltpu.VMEM(big, jnp.int32),
            pltpu.VMEM(big, jnp.int32),
            pltpu.VMEM(big, jnp.float32),
            pltpu.VMEM(big, jnp.float32),
            pltpu.VMEM(big, jnp.float32),
            pltpu.VMEM((ITERS - 2, 2, local, s), jnp.float32),
            pltpu.VMEM((s, k), jnp.float32),
            pltpu.VMEM((ITERS + 1, 8, s), jnp.float32),
            pltpu.VMEM((n, kr, s), TERM),
            pltpu.VMEM((n - 1, kr, s), TERM),
            pltpu.VMEM((s, k), jnp.float32),
            pltpu.VMEM((s, k), TERM),
            pltpu.VMEM((s, local), jnp.bfloat16),
            pltpu.VMEM((kr, s), jnp.float32),
            pltpu.VMEM((kr, s), jnp.bfloat16),
            pltpu.VMEM((n, kr, s), jnp.bfloat16),
            pltpu.VMEM((ITERS, s), jnp.float32),
            pltpu.VMEM((n, ITERS, s), jnp.float32),
            pltpu.VMEM((ITERS - 1, ITERS, s), jnp.float32),
            pltpu.SemaphoreType.DMA((6,)),
        ]
        + [dma] * 6,
        compiler_params=pltpu.CompilerParams(
            collective_id=0, has_side_effects=True, vmem_limit_bytes=42 * 1024 * 1024
        ),
        name="main",
    )(design_matrix, targets, linear, lines, lower_code, upper_code)
    return pl.pallas_call(
        functools.partial(mix_kernel, min(512, local)),
        in_specs=[vmem] * 4,
        out_specs=[hbm] * 2,
        out_shape=[jax.ShapeDtypeStruct(big, jnp.float32)] * 2,
        scratch_shapes=[
            pltpu.VMEM(big, jnp.float32),
            pltpu.VMEM(big, jnp.float32),
            pltpu.SemaphoreType.DMA((2, local // min(512, local))),
        ],
        compiler_params=pltpu.CompilerParams(vmem_limit_bytes=8 * 1024 * 1024),
        name="last_mix",
    )(mapped, alpha, lower, upper)


def solution(mesh):
    in_specs = (
        P("groups", "row"),
        P(("groups", "row"), None),
        P(("groups", "row"), None),
        P(("groups", "row")),
        P(("groups", "row"), None),
        P(("groups", "row"), None),
    )
    out_specs = (P(("groups", "row"), None), P(("groups", "row"), None))
    return jax.shard_map(
        functools.partial(per_device, mesh.shape["row"]),
        mesh=mesh,
        in_specs=in_specs,
        out_specs=out_specs,
        check_vma=False,
    )
```
